32 devices in a mesh: blk: 16 (over z, y, core), head: 2 (over x).
Axes of the slice: x: 2, y: 2, z: 4, core: 2. Of those that a mesh axis runs over, the one named last changes fastest.
Arguments:
- query_nope: bfloat16 [1024, 8192], P('blk', 'head'), may hold values from -140 to 140
- query_rope: bfloat16 [1024, 4096], P('blk', 'head'), may hold values from -6 to 6
- compressed: bfloat16 [1024, 576], P(('blk', 'head')), may hold values from -6 to 6
- latent_gain: float32 [512], replicated, may hold values from 0.1 to 1.9
- key_up: bfloat16 [64, 128, 512], P('head'), may hold values from -0.5 to 0.5
- value_up: bfloat16 [64, 512, 128], P('head'), may hold values from -1.5 to 1.5
- span_order: int32 [32], replicated, may hold values from 0 to 31, each once
Outputs:
- attended: bfloat16 [1024, 8192], P('blk', 'head')
The draws below stay inside these ranges and needn't reach their ends.
Inputs may be any that keep to these rules, and one draw needn't show every extreme that they name: Every number appears once; device index i of blk holds the blocks span_order[2 i] and span_order[2 i + 1].
All inputs are finite; a program needn't handle non-finite values.
Results may differ from the reference program's by a relative error of at most 0.0075.
The reference program's roundings to bfloat16 on the way count: a program that leaves them out, or rounds other values in their place, can miss the bound.
Values may be sent and summed in bfloat16 or wider, within the bound.
A program may use at most 64 MiB of HBM per device.

```python
import jax
import jax.numpy as jnp
from jax import lax

LATENT = 512
ROPE = 64
NOPE = 128
VDIM = 128
HEADS = 64
TOK_DEV = 64
TOKENS = 1024
N_BLK = 16


def draw_query_nope(key, part):
    first_key = jax.random.fold_in(jax.random.fold_in(key, 17), 0)
    values = jax.random.truncated_normal(first_key, -6.0, 6.0, (TOKENS, HEADS, NOPE), jnp.float32)
    return values.reshape(TOKENS, HEADS * NOPE).astype(jnp.bfloat16)


def block_levels(rng, dims, cuts, low, high):
    def one(position, blocks):
        steps = jax.random.uniform(jax.random.fold_in(jax.random.fold_in(rng, 6), position), (blocks,), jnp.float32, low / len(cuts), high / len(cuts))
        return jnp.repeat(jnp.exp(steps), dims[position] // blocks).reshape((-1,) + (1,) * (len(dims) - position - 1))

    loudness = one(*cuts[0])
    for cut in cuts[1:]:
        loudness = loudness * one(*cut)
    return loudness


def normal_values(own_key, shape, width, limit, cuts=(), kind=jnp.bfloat16):
    factor_of = block_levels(own_key, shape, cuts, -0.22, 0.18) if cuts else 1.0
    drawn = jax.random.normal(own_key, shape, jnp.float32) * width * factor_of
    return jnp.minimum(jnp.maximum(drawn, -limit), limit).astype(kind)


def setup_inputs(seed: int = 0) -> dict:
    arg_keys = jax.random.split(jax.random.key(seed), 8)
    return {
        "query_nope": draw_query_nope(jax.random.fold_in(arg_keys[7], 71), 0),
        "query_rope": normal_values(arg_keys[1], (TOKENS, HEADS * ROPE), 1.0, 6.0, ((0, 16), (1, 2))),
        "compressed": normal_values(arg_keys[2], (TOKENS, LATENT + ROPE), 1.0, 6.0, ((0, 32),)),
        "latent_gain": jnp.clip(1.0 + 0.18 * jax.random.normal(arg_keys[3], (LATENT,), jnp.float32), 0.1, 1.9),
        "key_up": normal_values(arg_keys[4], (HEADS, NOPE, LATENT), NOPE ** -0.5, 0.5, ((0, 2),)),
        "value_up": normal_values(arg_keys[5], (HEADS, LATENT, VDIM), (LATENT // 32) ** -0.5, 1.5, ((0, 2),)),
        "span_order": jax.random.permutation(arg_keys[6], 2 * N_BLK).astype(jnp.int32),
    }


norm_epsilon = 1e-06
rope_base = 10000.0
masked_score = -1e+30

def lookup(entries, index_array):
    slots = jnp.arange(entries.shape[0], dtype=jnp.int32)
    matches = index_array[..., None] == slots
    return lax.optimization_barrier(jnp.sum(jnp.where(matches, entries, 0), axis=-1)).astype(jnp.int32)

def rotate(values, positions):
    half_width = values.shape[-1] // 2
    frequency = rope_base ** (-jnp.arange(half_width, dtype=jnp.float32) / half_width)
    angles = positions.astype(jnp.float32)[..., None] * frequency
    cosine = jnp.cos(angles)
    sine_value = jnp.sin(angles)
    leading = values[..., :half_width]
    trailing = values[..., half_width:]
    return jnp.concatenate([leading * cosine - trailing * sine_value, leading * sine_value + trailing * cosine], axis=-1)

def reference(query_nope, query_rope, compressed, latent_gain, key_up, value_up, span_order):
    half_block = TOK_DEV // 2
    row_ids = jnp.arange(TOKENS, dtype=jnp.int32)
    positions = lookup(span_order, row_ids // half_block) * half_block + row_ids % half_block
    latent = compressed[:, :LATENT].astype(jnp.float32)
    latent = latent * lax.rsqrt(lax.optimization_barrier(jnp.mean(latent * latent, axis=1, keepdims=True)) + norm_epsilon) * latent_gain
    latent = latent.astype(jnp.bfloat16)
    key_rot = rotate(compressed[:, LATENT:].astype(jnp.float32), positions).astype(jnp.bfloat16)
    key_matrix = jnp.concatenate([latent, key_rot], axis=1)
    nope_parts = query_nope.reshape(TOKENS, HEADS, NOPE)
    query_rot = rotate(query_rope.reshape(TOKENS, HEADS, ROPE).astype(jnp.float32), positions[:, None]).astype(jnp.bfloat16)
    visible = positions[None, :] <= positions[:, None]
    score_scale = (NOPE + ROPE) ** (-0.5)

    def one_head(head_index):
        query_lat = jnp.dot(nope_parts[:, head_index, :], key_up[head_index], preferred_element_type=jnp.float32).astype(jnp.bfloat16)
        queries = jnp.concatenate([query_lat, query_rot[:, head_index, :]], axis=1)
        scores = jnp.dot(queries, key_matrix.T, preferred_element_type=jnp.float32) * score_scale
        scores = jnp.where(visible, scores, masked_score)
        row_max = lax.optimization_barrier(jnp.max(scores, axis=1, keepdims=True))
        weight = jnp.where(visible, jnp.exp(scores - row_max), 0.0)
        totals = lax.optimization_barrier(jnp.sum(weight, axis=1, keepdims=True))
        lat_out = jnp.dot(weight.astype(jnp.bfloat16), latent, preferred_element_type=jnp.float32) / totals
        lat_out = lat_out.astype(jnp.bfloat16)
        return jnp.dot(lat_out, value_up[head_index], preferred_element_type=jnp.float32).astype(jnp.bfloat16)
    outputs = lax.map(one_head, jnp.arange(HEADS, dtype=jnp.int32))
    return jnp.transpose(outputs, (1, 0, 2)).reshape(TOKENS, HEADS * VDIM)
```

```python
import functools
import math

import jax
import jax.numpy as jnp
import numpy as np
from jax import lax
from jax.experimental import pallas as pl
from jax.experimental.pallas import tpu as pltpu
from jax.sharding import PartitionSpec as P

norm_epsilon = 1e-06
rope_base = 10000.0
masked_score = -1e30
LANES = 128
GROUP = 8
LAG = 1
CHUNK = 256
MESH = pl.DeviceIdType.MESH


def rotate_tile(tile, cosine, signed_sine, rope_width):
    half = rope_width // 2
    width = tile.shape[-1]
    lane = lax.broadcasted_iota(jnp.int32, tile.shape, 1)
    partner = jnp.where(
        lane % rope_width < half,
        pltpu.roll(tile, width - half, 1),
        pltpu.roll(tile, half, 1),
    )
    return tile * cosine + partner * signed_sine


def angles_of(positions, freq, rope_width):
    angles = positions.astype(jnp.float32) * freq
    lane = lax.broadcasted_iota(jnp.int32, angles.shape, 1)
    sine = jnp.sin(angles)
    return jnp.cos(angles), jnp.where(lane % rope_width < rope_width // 2, -sine, sine)


def body(
    dims,
    remote,
    span_ref,
    keys_in_ref,
    gain_ref,
    freq_ref,
    nope_hbm,
    rope_hbm,
    key_up_hbm,
    value_up_hbm,
    out_ref,
    nope_ref,
    rope_ref,
    key_up_ref,
    value_up_ref,
    keys_ref,
    query_ref,
    mask_ref,
    acc_ref,
    top_ref,
    sum_ref,
    load_sem,
    send_sem,
    recv_sem,
    ready_sem,
):
    tokens, heads, nope, latent, rope, value, total, slices, chunk = dims
    half_block = tokens // 2
    scale = (nope + rope) ** (-0.5) * math.log2(math.e)
    blk = lax.axis_index("blk")
    head = lax.axis_index("head")
    chunks = total // chunk
    loads = [
        pltpu.make_async_copy(nope_hbm, nope_ref, load_sem.at[0]),
        pltpu.make_async_copy(rope_hbm, rope_ref, load_sem.at[1]),
        pltpu.make_async_copy(key_up_hbm, key_up_ref, load_sem.at[2]),
        pltpu.make_async_copy(value_up_hbm, value_up_ref, load_sem.at[3]),
    ]
    sends = []
    if remote:
        outer = lax.axis_size("blk") // 4
        o, i, c = blk // 4, (blk // 2) % 2, blk % 2

        def device(o_, i_, c_, h_):
            return ((o_ * 2 + i_) * 2 + c_, h_)

        def slot(o_, i_, c_, h_):
            return ((o_ * 2 + i_) * 2 + c_) * 2 + h_

        def block_at(index):
            return keys_ref.at[pl.ds(pl.multiple_of(index * slices, slices), slices)]

        def copy_to(index, target):
            copy = pltpu.make_async_remote_copy(
                src_ref=block_at(index),
                dst_ref=block_at(index),
                send_sem=send_sem.at[len(sends)],
                recv_sem=recv_sem.at[index],
                device_id=target,
                device_id_type=MESH,
            )
            sends.append(copy)
            return copy

        def arrive(index):
            pltpu.make_async_remote_copy(
                src_ref=block_at(index),
                dst_ref=block_at(index),
                send_sem=send_sem.at[0],
                recv_sem=recv_sem.at[index],
                device_id=sibling,
                device_id_type=MESH,
            ).wait_recv()

        def plane(k):
            return (k - 1) + ((k - 1) - o + outer) // outer

        sibling = device(o, i, 1 - c, head)
        corners = [(1 - i, 1 - head), (i, 1 - head), (1 - i, head)]
        flat = [device(o, i_, c, h_) for i_, h_ in corners]
        partners = [
            (device(plane(k), i, c, head), plane(k), o, plane(k) < o) for k in range(1, outer)
        ]
        for n, (peer, low) in enumerate(zip(flat + [sibling], (i == 1, head == 1, i == 1, c == 0))):
            partners.append((peer, outer + n, outer + n, low))
        barrier = pltpu.get_barrier_semaphore()
        for peer, _, _, low in partners:

            @pl.when(jnp.logical_not(low))
            def _():
                pl.semaphore_signal(barrier, inc=1, device_id=peer, device_id_type=MESH)

    for load in loads:
        load.start()

    if remote:
        first_row = blk * tokens + head * slices
        own_pos = (
            span_ref[first_row // half_block] * half_block
            + first_row % half_block
            + lax.broadcasted_iota(jnp.int32, (slices, LANES), 0)
        )
        own = keys_in_ref[...].astype(jnp.float32)
        own_latent = own[:, :latent]
        own_latent = (
            own_latent
            * lax.rsqrt(jnp.mean(own_latent * own_latent, axis=1, keepdims=True) + norm_epsilon)
            * gain_ref[...]
        )
        cosine, sine = angles_of(own_pos, freq_ref[...], rope)
        own_rope = own[:, latent : latent + rope]
        own_rope = jnp.concatenate([own_rope] * (LANES // rope), axis=1)
        own_slot = slot(o, i, c, head)
        own_block = block_at(own_slot)
        own_block[:, :latent] = own_latent.astype(jnp.bfloat16)
        own_block[:, latent:] = rotate_tile(own_rope, cosine, sine, rope).astype(jnp.bfloat16)

        ahead = o + head + 2 * i + (1 - c)

        @pl.when(ahead > 0)
        def _():
            pl.semaphore_wait(barrier, ahead)

        own_copies = [copy_to(own_slot, peer) for peer, _, _, _ in partners]
        for (peer, _, there, low), copy in zip(partners, own_copies):

            @pl.when(low)
            def _():
                pl.semaphore_signal(ready_sem.at[there], inc=1, device_id=peer, device_id_type=MESH)
                copy.start()

        def send_own(n):
            _, here, _, low = partners[n]

            @pl.when(jnp.logical_not(low))
            def _():
                pl.semaphore_wait(ready_sem.at[here], 1)
                own_copies[n].start()

    else:
        keys_copy = pltpu.make_async_copy(keys_in_ref, keys_ref, load_sem.at[4])
        keys_copy.start()

    token = lax.broadcasted_iota(jnp.int32, (tokens, LANES), 0)
    query_pos = (
        jnp.where(token < half_block, span_ref[blk * 2], span_ref[blk * 2 + 1]) * half_block
        + token % half_block
    )
    key_lane = lax.broadcasted_iota(jnp.int32, (8, total), 1)
    key_half = key_lane // half_block
    key_span = jnp.zeros((8, total), jnp.int32)
    for entry in range(total // half_block):
        key_span = jnp.where(key_half == entry, span_ref[entry], key_span)
    key_pos = key_span * half_block + key_lane % half_block
    mask = jnp.where(key_pos[:1] <= query_pos[:, :1], 0.0, masked_score)
    for n in range(chunks):
        mask_ref[n] = mask[:, n * chunk : (n + 1) * chunk]
    cosine, sine = angles_of(query_pos, freq_ref[...], rope)
    if remote:
        for n in (outer + 2, outer, outer + 1, outer - 1):
            send_own(n)
    loads[1].wait()
    per_tile = LANES // rope
    lane = lax.broadcasted_iota(jnp.int32, (tokens, LANES), 1)
    for tile in range(heads // per_tile):
        columns = rope_ref[:, tile * LANES : (tile + 1) * LANES].astype(jnp.float32)
        rotated = rotate_tile(columns, cosine, sine, rope)
        for part in range(per_tile):
            row = (tile * per_tile + part) * tokens
            query_ref[row : row + tokens, latent:] = jnp.where(
                lane // rope == part, rotated, 0.0
            ).astype(jnp.bfloat16)

    if remote:
        for k in range(1, outer):
            send_own(k - 1)
    loads[0].wait()
    loads[2].wait()
    for h in range(heads):
        query_ref[h * tokens : (h + 1) * tokens, :latent] = jnp.dot(
            nope_ref[:, h * nope : (h + 1) * nope],
            key_up_ref[h],
            preferred_element_type=jnp.float32,
        ).astype(jnp.bfloat16)

    group = min(GROUP, heads)
    rows = group * tokens

    def keys_of(n):
        return keys_ref.at[pl.ds(pl.multiple_of(n * chunk, chunk), chunk)]

    def scores_of(n, g):
        scores = lax.dot_general(
            query_ref[g * rows : (g + 1) * rows, :],
            keys_of(n)[...],
            (((1,), (1,)), ((), ())),
            preferred_element_type=jnp.float32,
        )
        return (scores.reshape(group, tokens, chunk) + mask_ref[n][None]).reshape(rows, chunk)

    def wide(array, width):
        return jnp.concatenate([array] * (width // LANES), axis=1)

    def weigh(n, g, scores, first, last):
        at = slice(g * rows, (g + 1) * rows)
        top = jnp.broadcast_to(jnp.max(scores, axis=1, keepdims=True), (rows, LANES))
        if not first:
            old = top_ref[at]
            top = jnp.maximum(top, old)
            fade = jnp.exp2((old - top) * scale)
        weight = jnp.exp2((scores - wide(top, chunk)) * scale)
        sums = weight[:, :LANES]
        for part in range(1, chunk // LANES):
            sums = sums + weight[:, part * LANES : (part + 1) * LANES]
        product = jnp.dot(
            weight.astype(jnp.bfloat16),
            keys_of(n)[:, :latent],
            preferred_element_type=jnp.float32,
        )
        if not first:
            sums = sums + sum_ref[at] * fade
            product = product + acc_ref[at] * wide(fade, latent)
        if not last:
            top_ref[at] = top
            sum_ref[at] = sums
            acc_ref[at] = product
            return
        share = 1.0 / jnp.sum(sums, axis=1, keepdims=True)
        lat_out = (product * share).astype(jnp.bfloat16)
        for m in range(group):
            h = g * group + m
            out_ref[:, h * value : (h + 1) * value] = jnp.dot(
                lat_out[m * tokens : (m + 1) * tokens],
                value_up_ref[h],
                preferred_element_type=jnp.float32,
            ).astype(jnp.bfloat16)

    def attend(n, first, last):
        waiting = []
        for g in range(heads // group):
            waiting.append((g, scores_of(n, g)))
            if len(waiting) > LAG:
                weigh(n, *waiting.pop(0), first, last)
        for entry in waiting:
            weigh(n, *entry, first, last)

    if remote:
        for k in range(1, outer):
            index = slot(plane(k), i, c, head)
            arrive(index)
            for peer in flat + [sibling]:
                copy_to(index, peer).start()

        def relay(p):
            for i_, h_ in corners[1:] + corners[:1]:
                index = slot(p, i_, c, h_)
                arrive(index)
                copy_to(index, sibling).start()

        def settle(p):
            for i_, h_ in [(i, head)] + corners[1:] + corners[:1]:
                arrive(slot(p, i_, 1 - c, h_))

        order = [o] + [plane(k) for k in range(1, outer)]
        relay(order[0])
        for n, p in enumerate(order):
            settle(p)
            last = n == outer - 1
            if last:
                loads[3].wait()
            attend(p, n == 0, last)
            if not last:
                relay(order[n + 1])
        for copy in sends:
            copy.wait_send()
    else:
        keys_copy.wait()
        loads[3].wait()
        if chunks == 1:
            attend(0, True, True)
        else:
            attend(0, True, False)

            def step(n, _):
                attend(n, False, False)
                return 0

            lax.fori_loop(1, chunks - 1, step, 0)
            attend(chunks - 1, False, True)


def shards(
    mesh, query_nope, query_rope, compressed, latent_gain, key_up, value_up, span_order
):
    tokens, (heads, nope, latent) = query_nope.shape[0], key_up.shape
    rope, value = query_rope.shape[1] // heads, value_up.shape[2]
    slices = compressed.shape[0]
    blocks, head_parts = mesh.shape["blk"], mesh.shape["head"]
    total = blocks * tokens
    half_block = tokens // 2
    half = rope // 2
    remote = head_parts == 2 and blocks % 4 == 0 and slices % 16 == 0 and half_block % slices == 0
    exponents = np.arange(LANES) % half
    freq = jnp.asarray((rope_base ** (-exponents / half)).astype(np.float32))[None]
    gain = latent_gain[None]
    if remote:
        keys_in = compressed
    else:
        rows = (
            lax.axis_index("blk") * tokens
            + lax.axis_index("head") * slices
            + jnp.arange(slices, dtype=jnp.int32)
        )
        pos = span_order[rows // half_block] * half_block + rows % half_block
        wide = compressed.astype(jnp.float32)
        lat = wide[:, :latent]
        lat = lat * lax.rsqrt(jnp.mean(lat * lat, axis=1, keepdims=True) + norm_epsilon) * gain
        angles = pos.astype(jnp.float32)[:, None] * freq[:, :half]
        a, b = wide[:, latent : latent + half], wide[:, latent + half :]
        cosine, sine = jnp.cos(angles), jnp.sin(angles)
        rot = [a * cosine - b * sine, a * sine + b * cosine]
        own = jnp.concatenate([lat] + rot * (LANES // rope), axis=1).astype(jnp.bfloat16)
        keys_in = lax.all_gather(own, ("blk", "head"), axis=0, tiled=True)
    any_space = pl.BlockSpec(memory_space=pl.ANY)
    rows = heads * tokens
    chunk = total // (blocks // 4) if remote else min(CHUNK, total)
    vmem = pl.BlockSpec(memory_space=pltpu.VMEM)
    dims = (tokens, heads, nope, latent, rope, value, total, slices, chunk)
    return pl.pallas_call(
        functools.partial(body, dims, remote),
        out_shape=pltpu.VMEM((tokens, heads * value), jnp.bfloat16),
        in_specs=[
            pl.BlockSpec(memory_space=pltpu.SMEM),
            vmem if remote else any_space,
            vmem,
            vmem,
            any_space,
            any_space,
            any_space,
            any_space,
        ],
        out_specs=vmem,
        scratch_shapes=[
            pltpu.VMEM(query_nope.shape, jnp.bfloat16),
            pltpu.VMEM(query_rope.shape, jnp.bfloat16),
            pltpu.VMEM(key_up.shape, jnp.bfloat16),
            pltpu.VMEM(value_up.shape, jnp.bfloat16),
            pltpu.VMEM((total, latent + LANES), jnp.bfloat16),
            pltpu.VMEM((rows, latent + LANES), jnp.bfloat16),
            pltpu.VMEM((total // chunk, tokens, chunk), jnp.float32),
            pltpu.VMEM((rows, latent), jnp.float32),
            pltpu.VMEM((rows, LANES), jnp.float32),
            pltpu.VMEM((rows, LANES), jnp.float32),
            pltpu.SemaphoreType.DMA((5,)),
            pltpu.SemaphoreType.DMA((2 * blocks if remote else 1,)),
            pltpu.SemaphoreType.DMA((2 * blocks if remote else 1,)),
            pltpu.SemaphoreType.REGULAR((blocks // 4 + 4,)),
        ],
        compiler_params=pltpu.CompilerParams(
            vmem_limit_bytes=60 * 1024 * 1024,
            has_side_effects=remote,
            **({"collective_id": 0} if remote else {}),
        ),
    )(span_order, keys_in, gain, freq, query_nope, query_rope, key_up, value_up)


def solution(mesh):
    in_specs = (
        P("blk", "head"),
        P("blk", "head"),
        P(("blk", "head"), None),
        P(),
        P("head", None, None),
        P("head", None, None),
        P(),
    )
    return jax.shard_map(
        functools.partial(shards, mesh),
        mesh=mesh,
        in_specs=in_specs,
        out_specs=P("blk", "head"),
        check_vma=False,
    )
```

```python
import functools
import math

import jax
import jax.numpy as jnp
import numpy as np
from jax import lax
from jax.experimental import pallas as pl
from jax.experimental.pallas import tpu as pltpu
from jax.sharding import PartitionSpec as P

norm_epsilon = 1e-06
rope_base = 10000.0
masked_score = -1e30
LANES = 128
GROUP = 8
LAG = 1
CHUNK = 256
MESH = pl.DeviceIdType.MESH


def rotate_tile(tile, cosine, signed_sine, rope_width):
    half = rope_width // 2
    width = tile.shape[-1]
    lane = lax.broadcasted_iota(jnp.int32, tile.shape, 1)
    partner = jnp.where(
        lane % rope_width < half,
        pltpu.roll(tile, width - half, 1),
        pltpu.roll(tile, half, 1),
    )
    return tile * cosine + partner * signed_sine


def angles_of(positions, freq, rope_width):
    angles = positions.astype(jnp.float32) * freq
    lane = lax.broadcasted_iota(jnp.int32, angles.shape, 1)
    sine = jnp.sin(angles)
    return jnp.cos(angles), jnp.where(lane % rope_width < rope_width // 2, -sine, sine)


def body(
    dims,
    remote,
    span_hbm,
    keys_in_hbm,
    gain_hbm,
    freq_hbm,
    nope_hbm,
    rope_hbm,
    key_up_hbm,
    value_up_hbm,
    out_ref,
    span_ref,
    keys_in_ref,
    gain_ref,
    freq_ref,
    nope_ref,
    rope_ref,
    key_up_ref,
    value_up_ref,
    wire_ref,
    keys_ref,
    query_ref,
    mask_ref,
    acc_ref,
    top_ref,
    sum_ref,
    part_ref,
    score_ref,
    load_sem,
    send_sem,
    recv_sem,
    ready_sem,
):
    tokens, heads, nope, latent, rope, value, total, slices, width = dims
    half_block = tokens // 2
    scale = (nope + rope) ** (-0.5) * math.log2(math.e)
    blk = lax.axis_index("blk")
    head = lax.axis_index("head")
    fields = total // width
    loads = [
        pltpu.make_async_copy(nope_hbm, nope_ref, load_sem.at[0]),
        pltpu.make_async_copy(rope_hbm, rope_ref, load_sem.at[1]),
        pltpu.make_async_copy(key_up_hbm, key_up_ref, load_sem.at[2]),
        pltpu.make_async_copy(value_up_hbm, value_up_ref, load_sem.at[3]),
    ]
    small = [
        pltpu.make_async_copy(span_hbm, span_ref, load_sem.at[5]),
        pltpu.make_async_copy(freq_hbm, freq_ref, load_sem.at[6]),
        pltpu.make_async_copy(gain_hbm, gain_ref, load_sem.at[7]),
    ]
    if remote:
        small.append(pltpu.make_async_copy(keys_in_hbm, keys_in_ref, load_sem.at[4]))
    sends = []
    if remote:
        outer = lax.axis_size("blk") // 4
        o, i, c = blk // 4, (blk // 2) % 2, blk % 2

        def device(o_, i_, c_, h_):
            return ((o_ * 2 + i_) * 2 + c_, h_)

        tiles = latent // LANES
        packed = slices * tiles + slices // 2
        def slot(o_, i_, c_, h_):
            return ((c_ * outer + o_) * 2 + i_) * 2 + h_

        def block_at(index):
            return wire_ref.at[pl.ds(pl.multiple_of(index * packed, 16), packed)]

        def line_of(p):
            return p

        def corner_of(p):
            return outer + p

        def sibling_of(p):
            return 2 * outer + p

        diagonal = 3 * outer
        counts = [0]

        def copy_to(index, target, landing, when=None):
            copy = pltpu.make_async_remote_copy(
                src_ref=block_at(index),
                dst_ref=block_at(index),
                send_sem=send_sem.at[0 if when is None else 1],
                recv_sem=recv_sem.at[landing],
                device_id=target,
                device_id_type=MESH,
            )
            if when is None:
                counts[0] += 1
            else:
                pl.when(when)(copy.start)
            return copy

        def arrive(landing, blocks):
            pltpu.make_async_remote_copy(
                src_ref=wire_ref.at[: blocks * packed],
                dst_ref=wire_ref.at[: blocks * packed],
                send_sem=send_sem.at[0],
                recv_sem=recv_sem.at[landing],
                device_id=sibling,
                device_id_type=MESH,
            ).wait_recv()

        def at_least(a, b):
            return (a - b + 2 * outer) // (2 * outer)

        above = outer - 1 - o
        upward = at_least(above, o)
        paired = o * upward + above * (1 - upward)

        def plane(k):
            near = at_least(2 * paired, k)
            by_turns = o - (k + 1) // 2 if k % 2 else o + k // 2
            onward = (o + k - paired) * upward + (o - k + paired) * (1 - upward)
            return by_turns * near + onward * (1 - near)

        sibling = device(o, i, 1 - c, head)
        corners = [(1 - i, 1 - head), (i, 1 - head), (1 - i, head)]
        flat = [device(o, i_, c, h_) for i_, h_ in corners]
        partners = []
        for n, (peer, low) in enumerate(zip(flat + [sibling], (i == 1, head == 1, i == 1, c == 0))):
            partners.append((peer, outer + n, outer + n, low))
        for k in range(1, outer):
            p = plane(k)
            partners.append((device(p, i, c, head), p, o, p < o))
        barrier = pltpu.get_barrier_semaphore()
        for peer, _, _, low in partners:

            @pl.when(jnp.logical_not(low))
            def _():
                pl.semaphore_signal(barrier, inc=1, device_id=peer, device_id_type=MESH)

    for load in small + loads:
        load.start()

    if remote:
        ahead = o + head + 2 * i + (1 - c)

        @pl.when(ahead > 0)
        def _():
            pl.semaphore_wait(barrier, ahead)

        for peer, _, there, low in partners:

            @pl.when(low)
            def _():
                pl.semaphore_signal(ready_sem.at[there], inc=1, device_id=peer, device_id_type=MESH)

        for load in small:
            load.wait()
        first_row = blk * tokens + head * slices
        own_pos = (
            span_ref[first_row // half_block] * half_block
            + first_row % half_block
            + lax.broadcasted_iota(jnp.int32, (slices, LANES), 0)
        )
        own = keys_in_ref[...].astype(jnp.float32)
        own_latent = own[:, :latent]
        own_latent = (
            own_latent
            * lax.rsqrt(jnp.mean(own_latent * own_latent, axis=1, keepdims=True) + norm_epsilon)
            * gain_ref[...]
        )
        cosine, sine = angles_of(own_pos, freq_ref[...], rope)
        own_rope = own[:, latent : latent + rope]
        own_rope = jnp.concatenate([own_rope] * (LANES // rope), axis=1)
        own_slot = slot(o, i, c, head)
        own_block = block_at(own_slot)
        for n in range(tiles):
            own_block[n * slices : (n + 1) * slices] = own_latent[
                :, n * LANES : (n + 1) * LANES
            ].astype(jnp.bfloat16)
        rotated = rotate_tile(own_rope, cosine, sine, rope)
        left = lax.broadcasted_iota(jnp.int32, (slices // 2, LANES), 1) < rope
        own_block[slices * tiles :] = jnp.where(
            left, rotated[: slices // 2], rotated[slices // 2 :]
        ).astype(jnp.bfloat16)

        def unpack(p):
            for c_ in range(2):
                for n in range(4):
                    index = (c_ * outer + p) * 4 + n
                    block = block_at(index)
                    row = pl.multiple_of(index * slices, slices)
                    for m in range(tiles):
                        keys_ref[pl.ds(row, slices), m * LANES : (m + 1) * LANES] = block[
                            m * slices : (m + 1) * slices
                        ]
                    pair = block[slices * tiles :].astype(jnp.float32)
                    turned = pltpu.roll(pair, rope, 1)
                    keys_ref[pl.ds(row, slices), latent:] = jnp.concatenate(
                        [jnp.where(left, pair, turned), jnp.where(left, turned, pair)], axis=0
                    ).astype(jnp.bfloat16)


        landings = [diagonal, corner_of(o), corner_of(o), sibling_of(o)] + [line_of(o)] * (outer - 1)
        own_copies = [
            copy_to(own_slot, peer, landing)
            for (peer, _, _, _), landing in zip(partners, landings)
        ]
        for (_, _, _, low), copy in reversed(list(zip(partners, own_copies))):
            pl.when(low)(copy.start)

        def send_own(n):
            _, here, _, low = partners[n]

            @pl.when(jnp.logical_not(low))
            def _():
                pl.semaphore_wait(ready_sem.at[here], 1)
                own_copies[n].start()

    else:
        for load in small:
            load.wait()
        keys_copy = pltpu.make_async_copy(keys_in_hbm, keys_ref, load_sem.at[4])
        keys_copy.start()

    token = lax.broadcasted_iota(jnp.int32, (tokens, LANES), 0)
    query_pos = (
        jnp.where(token < half_block, span_ref[blk * 2], span_ref[blk * 2 + 1]) * half_block
        + token % half_block
    )
    key_lane = lax.broadcasted_iota(jnp.int32, (8, total), 1)
    if remote:
        index = key_lane // slices
        key_row = (((index // 4) % outer * 2 + (index // 2) % 2) * 2 + index // (4 * outer)) * 2
        key_row = (key_row + index % 2) * slices + key_lane % slices
    else:
        key_row = key_lane
    key_half = key_row // half_block
    key_span = jnp.zeros((8, total), jnp.int32)
    for entry in range(total // half_block):
        key_span = jnp.where(key_half == entry, span_ref[entry], key_span)
    key_pos = key_span * half_block + key_row % half_block
    mask = jnp.where(key_pos[:1] <= query_pos[:, :1], 0.0, masked_score)
    for n in range(fields):
        mask_ref[n] = mask[:, n * width : (n + 1) * width]
    cosine, sine = angles_of(query_pos, freq_ref[...], rope)
    if remote:
        for n in (3, 1, 2, 0):
            send_own(n)
    loads[1].wait()
    per_tile = LANES // rope
    lane = lax.broadcasted_iota(jnp.int32, (tokens, LANES), 1)
    for tile in range(heads // per_tile):
        columns = rope_ref[:, tile * LANES : (tile + 1) * LANES].astype(jnp.float32)
        rotated = rotate_tile(columns, cosine, sine, rope)
        for part in range(per_tile):
            row = (tile * per_tile + part) * tokens
            query_ref[row : row + tokens, latent:] = jnp.where(
                lane // rope == part, rotated, 0.0
            ).astype(jnp.bfloat16)

    loads[0].wait()
    loads[2].wait()
    for h in range(heads):
        query_ref[h * tokens : (h + 1) * tokens, :latent] = jnp.dot(
            nope_ref[:, h * nope : (h + 1) * nope],
            key_up_ref[h],
            preferred_element_type=jnp.float32,
        ).astype(jnp.bfloat16)

    group = min(GROUP, heads)
    rows = group * tokens

    def keys_of(chunk, columns=latent + LANES):
        return jnp.concatenate(
            [
                keys_ref[pl.ds(pl.multiple_of(n * width, width), width), :columns]
                for n in chunk
            ],
            axis=0,
        )

    def scores_of(chunk, g):
        scores = lax.dot_general(
            query_ref[g * rows : (g + 1) * rows, :],
            keys_of(chunk),
            (((1,), (1,)), ((), ())),
            preferred_element_type=jnp.float32,
        )
        mask = jnp.concatenate([mask_ref[n] for n in chunk], axis=1)
        return (scores.reshape(group, tokens, -1) + mask[None]).reshape(rows, -1)

    def wide(array, columns):
        return jnp.concatenate([array] * (columns // LANES), axis=1)

    def finish(g, product, sums):
        share = 1.0 / jnp.sum(sums, axis=1, keepdims=True)
        lat_out = (product * share).astype(jnp.bfloat16)
        for m in range(group):
            h = g * group + m
            out_ref[:, h * value : (h + 1) * value] = jnp.dot(
                lat_out[m * tokens : (m + 1) * tokens],
                value_up_ref[h],
                preferred_element_type=jnp.float32,
            ).astype(jnp.bfloat16)

    def weigh(chunk, g, scores, first, last):
        keys = len(chunk) * width
        at = slice(g * rows, (g + 1) * rows)
        top = jnp.broadcast_to(jnp.max(scores, axis=1, keepdims=True), (rows, LANES))
        if not first:
            old = top_ref[at]
            top = jnp.maximum(top, old)
            fade = jnp.exp2((old - top) * scale)
        weight = jnp.exp2((scores - wide(top, keys)) * scale)
        sums = weight[:, :LANES]
        for part in range(1, keys // LANES):
            sums = sums + weight[:, part * LANES : (part + 1) * LANES]
        product = jnp.dot(
            weight.astype(jnp.bfloat16),
            keys_of(chunk, latent),
            preferred_element_type=jnp.float32,
        )
        if not first:
            sums = sums + sum_ref[at] * fade
            product = product + acc_ref[at] * wide(fade, latent)
        if not last:
            top_ref[at] = top
            sum_ref[at] = sums
            acc_ref[at] = product
            return
        finish(g, product, sums)

    def collect(chunk, at):
        for g in range(heads // group):
            scores = scores_of(chunk, g)
            where = slice(g * rows, (g + 1) * rows)
            score_ref[at, where] = scores
            part = part_ref[where] if at else top_ref[where]
            for n in range(len(chunk) * width // LANES):
                part = jnp.maximum(part, scores[:, n * LANES : (n + 1) * LANES])
            part_ref[where] = part

    def conclude(chunks):
        keys = sum(len(chunk) for chunk in chunks) * width
        values = [n for chunk in chunks for n in chunk]

        def weights(g):
            where = slice(g * rows, (g + 1) * rows)
            top = jnp.max(part_ref[where], axis=1, keepdims=True)
            top = jnp.broadcast_to(top, (rows, LANES))
            fade = jnp.exp2((top_ref[where] - top) * scale)
            scores = jnp.concatenate([score_ref[n, where] for n in range(len(chunks))], axis=1)
            weight = jnp.exp2((scores - wide(top, keys)) * scale)
            sums = sum_ref[where] * fade
            for n in range(keys // LANES):
                sums = sums + weight[:, n * LANES : (n + 1) * LANES]
            return g, weight.astype(jnp.bfloat16), fade, sums

        def close(g, weight, fade, sums):
            where = slice(g * rows, (g + 1) * rows)
            product = jnp.dot(weight, keys_of(values, latent), preferred_element_type=jnp.float32)
            finish(g, product + acc_ref[where] * wide(fade, latent), sums)

        ready = weights(0)
        for g in range(1, heads // group):
            following = weights(g)
            close(*ready)
            ready = following
        close(*ready)

    def attend(chunk, first, last, low=0, high=heads // group):
        waiting = []
        for g in range(low, high):
            waiting.append((g, scores_of(chunk, g)))
            if len(waiting) > LAG:
                weigh(chunk, *waiting.pop(0), first, last)
        for entry in waiting:
            weigh(chunk, *entry, first, last)

    if remote:

        def forward(p):
            index = slot(p, i, c, head)
            arrive(line_of(p), 1)
            for peer in flat[1:3]:
                copy_to(index, peer, corner_of(p)).start()
            copy_to(index, flat[0], corner_of(p), p < o - 1)
            copy_to(index, sibling, sibling_of(p)).start()

        def relay(p, at):
            arrive(corner_of(p), len(at))
            for i_, h_ in at:
                copy_to(slot(p, i_, c, h_), sibling, sibling_of(p)).start()

        half = heads // group // 2
        order = [o] + [plane(k) for k in range(1, outer)]
        others = order[1:]
        for n in range(4, len(partners)):
            send_own(n)
        across = slot(o, 1 - i, c, 1 - head)
        arrive(diagonal, 1)
        for p, (peer, _, _, _) in reversed(list(zip(others, partners[4:]))):
            copy_to(across, peer, corner_of(o), p < o + 2)
        copy_to(across, sibling, sibling_of(o)).start()
        relay(o, corners[1:])
        forward(others[0])
        arrive(sibling_of(o), 4)
        unpack(o)
        attend([o, outer + o], True, False, 0, half)
        for p in others[1:-1]:
            forward(p)
        attend([o, outer + o], True, False, half)
        forward(others[-1])

        numbers = [[p, outer + p] for p in others]
        relay(others[0], corners)
        arrive(sibling_of(others[0]), 4)
        unpack(others[0])
        collect(numbers[0], 0)
        for n in range(1, outer - 1):
            for p in others[1:3] if n == 1 else others[n + 1 : n + 2]:
                relay(p, corners)
            arrive(sibling_of(others[n]), 4)
            unpack(others[n])
            collect(numbers[n], n)
        loads[3].wait()
        conclude(numbers)

        def sent(blocks, at):
            pltpu.make_async_remote_copy(
                src_ref=wire_ref.at[: blocks * packed],
                dst_ref=wire_ref.at[: blocks * packed],
                send_sem=send_sem.at[at],
                recv_sem=recv_sem.at[0],
                device_id=sibling,
                device_id_type=MESH,
            ).wait_send()

        sent(counts[0], 0)
        for n in range(outer):
            taken = n + (n < outer - 1) + max(n - 1, 0)
            pl.when(o == n)(functools.partial(sent, taken, 1))
    else:
        keys_copy.wait()
        loads[3].wait()
        if fields == 1:
            attend([0], True, True)
        else:
            attend([0], True, False)

            def step(n, _):
                attend([n], False, False)
                return 0

            lax.fori_loop(1, fields - 1, step, 0)
            attend([fields - 1], False, True)


def shards(
    mesh, query_nope, query_rope, compressed, latent_gain, key_up, value_up, span_order
):
    tokens, (heads, nope, latent) = query_nope.shape[0], key_up.shape
    rope, value = query_rope.shape[1] // heads, value_up.shape[2]
    slices = compressed.shape[0]
    blocks, head_parts = mesh.shape["blk"], mesh.shape["head"]
    total = blocks * tokens
    half_block = tokens // 2
    half = rope // 2
    remote = head_parts == 2 and blocks % 4 == 0 and blocks >= 16 and slices % 32 == 0 and half_block % slices == 0 and 2 * rope == LANES
    exponents = np.arange(LANES) % half
    freq = jnp.asarray((rope_base ** (-exponents / half)).astype(np.float32))[None]
    gain = latent_gain[None]
    if remote:
        keys_in = compressed
    else:
        rows = (
            lax.axis_index("blk") * tokens
            + lax.axis_index("head") * slices
            + jnp.arange(slices, dtype=jnp.int32)
        )
        pos = span_order[rows // half_block] * half_block + rows % half_block
        wide = compressed.astype(jnp.float32)
        lat = wide[:, :latent]
        lat = lat * lax.rsqrt(jnp.mean(lat * lat, axis=1, keepdims=True) + norm_epsilon) * gain
        angles = pos.astype(jnp.float32)[:, None] * freq[:, :half]
        a, b = wide[:, latent : latent + half], wide[:, latent + half :]
        cosine, sine = jnp.cos(angles), jnp.sin(angles)
        rot = [a * cosine - b * sine, a * sine + b * cosine]
        own = jnp.concatenate([lat] + rot * (LANES // rope), axis=1).astype(jnp.bfloat16)
        keys_in = lax.all_gather(own, ("blk", "head"), axis=0, tiled=True)
    any_space = pl.BlockSpec(memory_space=pl.ANY)
    rows = heads * tokens
    wire_rows = 2 * blocks * slices * (2 * latent + LANES) // (2 * LANES) if remote else 16
    width = 4 * slices if remote else min(CHUNK, total)
    vmem = pl.BlockSpec(memory_space=pltpu.VMEM)
    dims = (tokens, heads, nope, latent, rope, value, total, slices, width)
    return pl.pallas_call(
        functools.partial(body, dims, remote),
        out_shape=pltpu.VMEM((tokens, heads * value), jnp.bfloat16),
        in_specs=[
            any_space,
            any_space,
            any_space,
            any_space,
            any_space,
            any_space,
            any_space,
            any_space,
        ],
        out_specs=vmem,
        scratch_shapes=[
            pltpu.SMEM(span_order.shape, jnp.int32),
            pltpu.VMEM(compressed.shape, jnp.bfloat16),
            pltpu.VMEM(gain.shape, jnp.float32),
            pltpu.VMEM(freq.shape, jnp.float32),
            pltpu.VMEM(query_nope.shape, jnp.bfloat16),
            pltpu.VMEM(query_rope.shape, jnp.bfloat16),
            pltpu.VMEM(key_up.shape, jnp.bfloat16),
            pltpu.VMEM(value_up.shape, jnp.bfloat16),
            pltpu.VMEM((wire_rows, LANES), jnp.bfloat16),
            pltpu.VMEM((total, latent + LANES), jnp.bfloat16),
            pltpu.VMEM((rows, latent + LANES), jnp.bfloat16),
            pltpu.VMEM((total // width, tokens, width), jnp.float32),
            pltpu.VMEM((rows, latent), jnp.float32),
            pltpu.VMEM((rows, LANES), jnp.float32),
            pltpu.VMEM((rows, LANES), jnp.float32),
            pltpu.VMEM((rows, LANES), jnp.float32),
            pltpu.VMEM((blocks // 4 - 1, rows, 2 * width) if remote else (1, 8, LANES), jnp.float32),
            pltpu.SemaphoreType.DMA((8,)),
            pltpu.SemaphoreType.DMA((2,)),
            pltpu.SemaphoreType.DMA((3 * (blocks // 4) + 1 if remote else 1,)),
            pltpu.SemaphoreType.REGULAR((blocks // 4 + 4,)),
        ],
        compiler_params=pltpu.CompilerParams(
            vmem_limit_bytes=60 * 1024 * 1024,
            has_side_effects=remote,
            **({"collective_id": 0} if remote else {}),
        ),
    )(span_order, keys_in, gain, freq, query_nope, query_rope, key_up, value_up)


def solution(mesh):
    in_specs = (
        P("blk", "head"),
        P("blk", "head"),
        P(("blk", "head"), None),
        P(),
        P("head", None, None),
        P("head", None, None),
        P(),
    )
    return jax.shard_map(
        functools.partial(shards, mesh),
        mesh=mesh,
        in_specs=in_specs,
        out_specs=P("blk", "head"),
        check_vma=False,
    )
```

```python
import functools
import math

import jax
import jax.numpy as jnp
import numpy as np
from jax import lax
from jax.experimental import pallas as pl
from jax.experimental.pallas import tpu as pltpu
from jax.sharding import PartitionSpec as P

norm_epsilon = 1e-06
rope_base = 10000.0
masked_score = -1e30
LANES = 128
GROUP = 8
LAG = 1
CHUNK = 256
MESH = pl.DeviceIdType.MESH


def rotate_tile(tile, cosine, signed_sine, rope_width):
    half = rope_width // 2
    width = tile.shape[-1]
    lane = lax.broadcasted_iota(jnp.int32, tile.shape, 1)
    partner = jnp.where(
        lane % rope_width < half,
        pltpu.roll(tile, width - half, 1),
        pltpu.roll(tile, half, 1),
    )
    return tile * cosine + partner * signed_sine


def angles_of(positions, freq, rope_width):
    angles = positions.astype(jnp.float32) * freq
    lane = lax.broadcasted_iota(jnp.int32, angles.shape, 1)
    sine = jnp.sin(angles)
    return jnp.cos(angles), jnp.where(lane % rope_width < rope_width // 2, -sine, sine)


def body(
    dims,
    remote,
    span_hbm,
    keys_in_hbm,
    gain_hbm,
    freq_hbm,
    nope_hbm,
    rope_hbm,
    key_up_hbm,
    value_up_hbm,
    out_ref,
    span_ref,
    keys_in_ref,
    gain_ref,
    freq_ref,
    nope_ref,
    rope_ref,
    key_up_ref,
    value_up_ref,
    wire_ref,
    keys_ref,
    query_ref,
    mask_ref,
    acc_ref,
    top_ref,
    sum_ref,
    part_ref,
    score_ref,
    load_sem,
    send_sem,
    recv_sem,
    ready_sem,
):
    tokens, heads, nope, latent, rope, value, total, slices, width = dims
    half_block = tokens // 2
    scale = (nope + rope) ** (-0.5) * math.log2(math.e)
    blk = lax.axis_index("blk")
    head = lax.axis_index("head")
    fields = total // width
    loads = [
        pltpu.make_async_copy(nope_hbm, nope_ref, load_sem.at[0]),
        pltpu.make_async_copy(rope_hbm, rope_ref, load_sem.at[1]),
        pltpu.make_async_copy(key_up_hbm, key_up_ref, load_sem.at[2]),
        pltpu.make_async_copy(value_up_hbm, value_up_ref, load_sem.at[3]),
    ]
    small = [
        pltpu.make_async_copy(span_hbm, span_ref, load_sem.at[5]),
        pltpu.make_async_copy(freq_hbm, freq_ref, load_sem.at[6]),
        pltpu.make_async_copy(gain_hbm, gain_ref, load_sem.at[7]),
    ]
    if remote:
        small.append(pltpu.make_async_copy(keys_in_hbm, keys_in_ref, load_sem.at[4]))
    sends = []
    if remote:
        outer = lax.axis_size("blk") // 4
        o, i, c = blk // 4, (blk // 2) % 2, blk % 2

        def device(o_, i_, c_, h_):
            return ((o_ * 2 + i_) * 2 + c_, h_)

        tiles = latent // LANES
        packed = slices * tiles + slices // 2
        def slot(o_, i_, c_, h_):
            return ((c_ * outer + o_) * 2 + i_) * 2 + h_

        def block_at(index):
            return wire_ref.at[pl.ds(pl.multiple_of(index * packed, 16), packed)]

        def line_of(p):
            return p

        def corner_of(p):
            return outer + p

        def sibling_of(p):
            return 2 * outer + p

        diagonal = 3 * outer
        counts = [0]

        def copy_to(index, target, landing, when=None):
            copy = pltpu.make_async_remote_copy(
                src_ref=block_at(index),
                dst_ref=block_at(index),
                send_sem=send_sem.at[0 if when is None else 1],
                recv_sem=recv_sem.at[landing],
                device_id=target,
                device_id_type=MESH,
            )
            if when is None:
                counts[0] += 1
            else:
                pl.when(when)(copy.start)
            return copy

        def arrive(landing, blocks):
            pltpu.make_async_remote_copy(
                src_ref=wire_ref.at[: blocks * packed],
                dst_ref=wire_ref.at[: blocks * packed],
                send_sem=send_sem.at[0],
                recv_sem=recv_sem.at[landing],
                device_id=sibling,
                device_id_type=MESH,
            ).wait_recv()

        def at_least(a, b):
            return (a - b + 2 * outer) // (2 * outer)

        above = outer - 1 - o
        upward = at_least(above, o)
        paired = o * upward + above * (1 - upward)

        def plane(k):
            near = at_least(2 * paired, k)
            by_turns = o - (k + 1) // 2 if k % 2 else o + k // 2
            onward = (o + k - paired) * upward + (o - k + paired) * (1 - upward)
            return by_turns * near + onward * (1 - near)

        sibling = device(o, i, 1 - c, head)
        corners = [(1 - i, 1 - head), (i, 1 - head), (1 - i, head)]
        flat = [device(o, i_, c, h_) for i_, h_ in corners]
        partners = []
        for n, (peer, low) in enumerate(zip(flat + [sibling], (i == 1, head == 1, i == 1, c == 0))):
            partners.append((peer, outer + n, outer + n, low))
        for k in range(1, outer):
            p = plane(k)
            partners.append((device(p, i, c, head), p, o, p < o))
        barrier = pltpu.get_barrier_semaphore()
        for peer, _, _, low in partners:

            @pl.when(jnp.logical_not(low))
            def _():
                pl.semaphore_signal(barrier, inc=1, device_id=peer, device_id_type=MESH)

    for load in small + loads:
        load.start()

    if remote:
        ahead = o + head + 2 * i + (1 - c)

        @pl.when(ahead > 0)
        def _():
            pl.semaphore_wait(barrier, ahead)

        for peer, _, there, low in partners:

            @pl.when(low)
            def _():
                pl.semaphore_signal(ready_sem.at[there], inc=1, device_id=peer, device_id_type=MESH)

        for load in small:
            load.wait()
        first_row = blk * tokens + head * slices
        own_pos = (
            span_ref[first_row // half_block] * half_block
            + first_row % half_block
            + lax.broadcasted_iota(jnp.int32, (slices, LANES), 0)
        )
        own = keys_in_ref[...].astype(jnp.float32)
        own_latent = own[:, :latent]
        own_latent = (
            own_latent
            * lax.rsqrt(jnp.mean(own_latent * own_latent, axis=1, keepdims=True) + norm_epsilon)
            * gain_ref[...]
        )
        cosine, sine = angles_of(own_pos, freq_ref[...], rope)
        own_rope = own[:, latent : latent + rope]
        own_rope = jnp.concatenate([own_rope] * (LANES // rope), axis=1)
        own_slot = slot(o, i, c, head)
        own_block = block_at(own_slot)
        for n in range(tiles):
            own_block[n * slices : (n + 1) * slices] = own_latent[
                :, n * LANES : (n + 1) * LANES
            ].astype(jnp.bfloat16)
        rotated = rotate_tile(own_rope, cosine, sine, rope)
        left = lax.broadcasted_iota(jnp.int32, (slices // 2, LANES), 1) < rope
        own_block[slices * tiles :] = jnp.where(
            left, rotated[: slices // 2], rotated[slices // 2 :]
        ).astype(jnp.bfloat16)

        def unpack(p):
            for c_ in range(2):
                for n in range(4):
                    index = (c_ * outer + p) * 4 + n
                    block = block_at(index)
                    row = pl.multiple_of(index * slices, slices)
                    for m in range(tiles):
                        keys_ref[pl.ds(row, slices), m * LANES : (m + 1) * LANES] = block[
                            m * slices : (m + 1) * slices
                        ]
                    pair = block[slices * tiles :].astype(jnp.float32)
                    turned = pltpu.roll(pair, rope, 1)
                    keys_ref[pl.ds(row, slices), latent:] = jnp.concatenate(
                        [jnp.where(left, pair, turned), jnp.where(left, turned, pair)], axis=0
                    ).astype(jnp.bfloat16)


        landings = [diagonal, corner_of(o), corner_of(o), sibling_of(o)] + [line_of(o)] * (outer - 1)
        own_copies = [
            copy_to(own_slot, peer, landing)
            for (peer, _, _, _), landing in zip(partners, landings)
        ]
        for (_, _, _, low), copy in reversed(list(zip(partners, own_copies))):
            pl.when(low)(copy.start)

        def send_own(n):
            _, here, _, low = partners[n]

            @pl.when(jnp.logical_not(low))
            def _():
                pl.semaphore_wait(ready_sem.at[here], 1)
                own_copies[n].start()

    else:
        for load in small:
            load.wait()
        keys_copy = pltpu.make_async_copy(keys_in_hbm, keys_ref, load_sem.at[4])
        keys_copy.start()

    token = lax.broadcasted_iota(jnp.int32, (tokens, LANES), 0)
    query_pos = (
        jnp.where(token < half_block, span_ref[blk * 2], span_ref[blk * 2 + 1]) * half_block
        + token % half_block
    )
    key_lane = lax.broadcasted_iota(jnp.int32, (8, total), 1)
    if remote:
        index = key_lane // slices
        key_row = (((index // 4) % outer * 2 + (index // 2) % 2) * 2 + index // (4 * outer)) * 2
        key_row = (key_row + index % 2) * slices + key_lane % slices
    else:
        key_row = key_lane
    key_half = key_row // half_block
    key_span = jnp.zeros((8, total), jnp.int32)
    for entry in range(total // half_block):
        key_span = jnp.where(key_half == entry, span_ref[entry], key_span)
    key_pos = key_span * half_block + key_row % half_block
    mask = jnp.where(key_pos[:1] <= query_pos[:, :1], 0.0, masked_score)
    for n in range(fields):
        mask_ref[n] = mask[:, n * width : (n + 1) * width]
    cosine, sine = angles_of(query_pos, freq_ref[...], rope)
    if remote:
        for n in (3, 1, 2, 0):
            send_own(n)
    loads[1].wait()
    per_tile = LANES // rope
    lane = lax.broadcasted_iota(jnp.int32, (tokens, LANES), 1)
    for tile in range(heads // per_tile):
        columns = rope_ref[:, tile * LANES : (tile + 1) * LANES].astype(jnp.float32)
        rotated = rotate_tile(columns, cosine, sine, rope)
        for part in range(per_tile):
            row = (tile * per_tile + part) * tokens
            query_ref[row : row + tokens, latent:] = jnp.where(
                lane // rope == part, rotated, 0.0
            ).astype(jnp.bfloat16)

    loads[0].wait()
    loads[2].wait()
    for h in range(heads):
        query_ref[h * tokens : (h + 1) * tokens, :latent] = jnp.dot(
            nope_ref[:, h * nope : (h + 1) * nope],
            key_up_ref[h],
            preferred_element_type=jnp.float32,
        ).astype(jnp.bfloat16)

    group = min(GROUP, heads)
    rows = group * tokens

    def keys_of(chunk, columns=latent + LANES):
        return jnp.concatenate(
            [
                keys_ref[pl.ds(pl.multiple_of(n * width, width), width), :columns]
                for n in chunk
            ],
            axis=0,
        )

    def scores_of(chunk, g):
        scores = lax.dot_general(
            query_ref[g * rows : (g + 1) * rows, :],
            keys_of(chunk),
            (((1,), (1,)), ((), ())),
            preferred_element_type=jnp.float32,
        )
        mask = jnp.concatenate([mask_ref[n] for n in chunk], axis=1)
        return (scores.reshape(group, tokens, -1) + mask[None]).reshape(rows, -1)

    def wide(array, columns):
        return jnp.concatenate([array] * (columns // LANES), axis=1)

    def finish(g, product, sums):
        share = 1.0 / jnp.sum(sums, axis=1, keepdims=True)
        lat_out = (product * share).astype(jnp.bfloat16)
        for m in range(group):
            h = g * group + m
            out_ref[:, h * value : (h + 1) * value] = jnp.dot(
                lat_out[m * tokens : (m + 1) * tokens],
                value_up_ref[h],
                preferred_element_type=jnp.float32,
            ).astype(jnp.bfloat16)

    def weigh(chunk, g, scores, first, last):
        keys = len(chunk) * width
        at = slice(g * rows, (g + 1) * rows)
        top = jnp.broadcast_to(jnp.max(scores, axis=1, keepdims=True), (rows, LANES))
        if not first:
            old = top_ref[at]
            top = jnp.maximum(top, old)
            fade = jnp.exp2((old - top) * scale)
        weight = jnp.exp2((scores - wide(top, keys)) * scale)
        sums = weight[:, :LANES]
        for part in range(1, keys // LANES):
            sums = sums + weight[:, part * LANES : (part + 1) * LANES]
        product = jnp.dot(
            weight.astype(jnp.bfloat16),
            keys_of(chunk, latent),
            preferred_element_type=jnp.float32,
        )
        if not first:
            sums = sums + sum_ref[at] * fade
            product = product + acc_ref[at] * wide(fade, latent)
        if not last:
            top_ref[at] = top
            sum_ref[at] = sums
            acc_ref[at] = product
            return
        finish(g, product, sums)

    def collect(chunk, at):
        for g in range(heads // group):
            scores = scores_of(chunk, g)
            where = slice(g * rows, (g + 1) * rows)
            score_ref[at, where] = scores
            part = part_ref[where] if at else top_ref[where]
            for n in range(len(chunk) * width // LANES):
                part = jnp.maximum(part, scores[:, n * LANES : (n + 1) * LANES])
            part_ref[where] = part

    def conclude(chunks):
        values = [n for chunk in chunks for n in chunk]
        keys = len(values) * width
        for g in range(heads // group):
            where = slice(g * rows, (g + 1) * rows)
            top = jnp.max(part_ref[where], axis=1, keepdims=True)
            top = jnp.broadcast_to(top, (rows, LANES))
            fade = jnp.exp2((top_ref[where] - top) * scale)
            scores = jnp.concatenate([score_ref[n, where] for n in range(len(chunks))], axis=1)
            weight = jnp.exp2((scores - wide(top, keys)) * scale)
            sums = sum_ref[where] * fade
            for n in range(keys // LANES):
                sums = sums + weight[:, n * LANES : (n + 1) * LANES]
            product = jnp.dot(
                weight.astype(jnp.bfloat16),
                keys_of(values, latent),
                preferred_element_type=jnp.float32,
            )
            finish(g, product + acc_ref[where] * wide(fade, latent), sums)

    def attend(chunk, first, last, low=0, high=heads // group):
        waiting = []
        for g in range(low, high):
            waiting.append((g, scores_of(chunk, g)))
            if len(waiting) > LAG:
                weigh(chunk, *waiting.pop(0), first, last)
        for entry in waiting:
            weigh(chunk, *entry, first, last)

    if remote:

        def forward(p):
            index = slot(p, i, c, head)
            arrive(line_of(p), 1)
            for peer in flat[1:3]:
                copy_to(index, peer, corner_of(p)).start()
            copy_to(index, flat[0], corner_of(p), p < o - 1)
            copy_to(index, sibling, sibling_of(p)).start()

        def relay(p, at):
            arrive(corner_of(p), len(at))
            for i_, h_ in at:
                copy_to(slot(p, i_, c, h_), sibling, sibling_of(p)).start()

        half = heads // group // 2
        others = [plane(k) for k in range(1, outer)]
        numbers = [[p, outer + p] for p in [o] + others]
        for n in range(4, len(partners)):
            send_own(n)
        across = slot(o, 1 - i, c, 1 - head)
        arrive(diagonal, 1)
        for p, (peer, _, _, _) in reversed(list(zip(others, partners[4:]))):
            copy_to(across, peer, corner_of(o), p < o + 2)
        copy_to(across, sibling, sibling_of(o)).start()
        relay(o, corners[1:])
        late = jnp.logical_and(o == outer - 1, c == 0)
        counted = counts[0]

        @pl.when(jnp.logical_not(late))
        def _():
            forward(others[0])

        counts[0] = counted
        arrive(sibling_of(o), 4)
        unpack(o)
        attend(numbers[0], True, False, 0, half)

        @pl.when(late)
        def _():
            forward(others[0])

        for p in others[1:-1]:
            forward(p)
        attend(numbers[0], True, False, half)
        forward(others[-1])
        relay(others[0], corners)
        arrive(sibling_of(others[0]), 4)
        unpack(others[0])
        attend(numbers[1], False, False, 0, half)
        relay(others[1], corners)
        attend(numbers[1], False, False, half)
        for n in range(1, outer - 1):
            if n + 1 < outer - 1:
                relay(others[n + 1], corners)
            arrive(sibling_of(others[n]), 4)
            unpack(others[n])
            collect(numbers[n + 1], n - 1)
        loads[3].wait()
        conclude(numbers[2:])

        def sent(blocks, at):
            pltpu.make_async_remote_copy(
                src_ref=wire_ref.at[: blocks * packed],
                dst_ref=wire_ref.at[: blocks * packed],
                send_sem=send_sem.at[at],
                recv_sem=recv_sem.at[0],
                device_id=sibling,
                device_id_type=MESH,
            ).wait_send()

        sent(counts[0], 0)
        for n in range(outer):
            taken = n + (n < outer - 1) + max(n - 1, 0)
            pl.when(o == n)(functools.partial(sent, taken, 1))
    else:
        keys_copy.wait()
        loads[3].wait()
        if fields == 1:
            attend([0], True, True)
        else:
            attend([0], True, False)

            def step(n, _):
                attend([n], False, False)
                return 0

            lax.fori_loop(1, fields - 1, step, 0)
            attend([fields - 1], False, True)


def shards(
    mesh, query_nope, query_rope, compressed, latent_gain, key_up, value_up, span_order
):
    tokens, (heads, nope, latent) = query_nope.shape[0], key_up.shape
    rope, value = query_rope.shape[1] // heads, value_up.shape[2]
    slices = compressed.shape[0]
    blocks, head_parts = mesh.shape["blk"], mesh.shape["head"]
    total = blocks * tokens
    half_block = tokens // 2
    half = rope // 2
    remote = head_parts == 2 and blocks % 4 == 0 and blocks >= 16 and slices % 32 == 0 and half_block % slices == 0 and 2 * rope == LANES
    exponents = np.arange(LANES) % half
    freq = jnp.asarray((rope_base ** (-exponents / half)).astype(np.float32))[None]
    gain = latent_gain[None]
    if remote:
        keys_in = compressed
    else:
        rows = (
            lax.axis_index("blk") * tokens
            + lax.axis_index("head") * slices
            + jnp.arange(slices, dtype=jnp.int32)
        )
        pos = span_order[rows // half_block] * half_block + rows % half_block
        wide = compressed.astype(jnp.float32)
        lat = wide[:, :latent]
        lat = lat * lax.rsqrt(jnp.mean(lat * lat, axis=1, keepdims=True) + norm_epsilon) * gain
        angles = pos.astype(jnp.float32)[:, None] * freq[:, :half]
        a, b = wide[:, latent : latent + half], wide[:, latent + half :]
        cosine, sine = jnp.cos(angles), jnp.sin(angles)
        rot = [a * cosine - b * sine, a * sine + b * cosine]
        own = jnp.concatenate([lat] + rot * (LANES // rope), axis=1).astype(jnp.bfloat16)
        keys_in = lax.all_gather(own, ("blk", "head"), axis=0, tiled=True)
    any_space = pl.BlockSpec(memory_space=pl.ANY)
    rows = heads * tokens
    wire_rows = 2 * blocks * slices * (2 * latent + LANES) // (2 * LANES) if remote else 16
    width = 4 * slices if remote else min(CHUNK, total)
    vmem = pl.BlockSpec(memory_space=pltpu.VMEM)
    dims = (tokens, heads, nope, latent, rope, value, total, slices, width)
    return pl.pallas_call(
        functools.partial(body, dims, remote),
        out_shape=pltpu.VMEM((tokens, heads * value), jnp.bfloat16),
        in_specs=[
            any_space,
            any_space,
            any_space,
            any_space,
            any_space,
            any_space,
            any_space,
            any_space,
        ],
        out_specs=vmem,
        scratch_shapes=[
            pltpu.SMEM(span_order.shape, jnp.int32),
            pltpu.VMEM(compressed.shape, jnp.bfloat16),
            pltpu.VMEM(gain.shape, jnp.float32),
            pltpu.VMEM(freq.shape, jnp.float32),
            pltpu.VMEM(query_nope.shape, jnp.bfloat16),
            pltpu.VMEM(query_rope.shape, jnp.bfloat16),
            pltpu.VMEM(key_up.shape, jnp.bfloat16),
            pltpu.VMEM(value_up.shape, jnp.bfloat16),
            pltpu.VMEM((wire_rows, LANES), jnp.bfloat16),
            pltpu.VMEM((total, latent + LANES), jnp.bfloat16),
            pltpu.VMEM((rows, latent + LANES), jnp.bfloat16),
            pltpu.VMEM((total // width, tokens, width), jnp.float32),
            pltpu.VMEM((rows, latent), jnp.float32),
            pltpu.VMEM((rows, LANES), jnp.float32),
            pltpu.VMEM((rows, LANES), jnp.float32),
            pltpu.VMEM((rows, LANES), jnp.float32),
            pltpu.VMEM((blocks // 4 - 2, rows, 2 * width) if remote else (1, 8, LANES), jnp.float32),
            pltpu.SemaphoreType.DMA((8,)),
            pltpu.SemaphoreType.DMA((2,)),
            pltpu.SemaphoreType.DMA((3 * (blocks // 4) + 1 if remote else 1,)),
            pltpu.SemaphoreType.REGULAR((blocks // 4 + 4,)),
        ],
        compiler_params=pltpu.CompilerParams(
            vmem_limit_bytes=60 * 1024 * 1024,
            has_side_effects=remote,
            **({"collective_id": 0} if remote else {}),
        ),
    )(span_order, keys_in, gain, freq, query_nope, query_rope, key_up, value_up)


def solution(mesh):
    in_specs = (
        P("blk", "head"),
        P("blk", "head"),
        P(("blk", "head"), None),
        P(),
        P("head", None, None),
        P("head", None, None),
        P(),
    )
    return jax.shard_map(
        functools.partial(shards, mesh),
        mesh=mesh,
        in_specs=in_specs,
        out_specs=P("blk", "head"),
        check_vma=False,
    )
```
